32 devices in a mesh: dp: 4 (over y, x), expert: 8 (over z, core).
Axes of the slice: x: 2, y: 2, z: 4, core: 2. Of those that a mesh axis runs over, the one named last changes fastest.
Arguments:
- tokens: bfloat16 [8192, 2048], P(('dp', 'expert')), may hold values from -6 to 6
- expert_ids: int32 [8192, 8], P(('dp', 'expert')), may hold values from 0 to 15, all different within a row; in each aligned block of 256 rows (0 to 255, 256 to 511, ...) at most 160 rows name the same one
- route_probs: float32 [8192, 8], P(('dp', 'expert')), may hold values from 0.05 to 1
- w_gate_up: bfloat16 [16, 2048, 1536], P('expert', 'dp'), may hold values from -0.125 to 0.125
- w_down: bfloat16 [16, 768, 2048], P('expert', None, 'dp'), may hold values from -0.21875 to 0.21875
Outputs:
- moe_out: bfloat16 [8192, 2048], P(('dp', 'expert'))
The draws below stay inside these ranges and needn't reach their ends.
Inputs may be any that keep to these rules, and one draw needn't show every extreme that they name: `expert_ids`: each row names 8 different experts. Among the rows of one device no expert is named more than 160 times, and in every draw some expert is named exactly 160 times in some device's rows.
All inputs are finite; a program needn't handle non-finite values.
Results may differ from the reference program's by a relative error of at most 0.0057.
Values may be sent and summed in bfloat16 or wider, within the bound.
A program may use at most 128 MiB of HBM per device.

```python
import math
import jax
import jax.numpy as jnp
import numpy as np
from jax import lax

D = 2048
FF = 768
TOP = 8
TOK_DEV = 256
EXPERTS = 16
CAP = 160
TOKENS = 8192


def levels(rng, dims, split, smallest, high):
    gain = 1.0
    for axis_at, blocks in split:
        heights = jax.random.uniform(jax.random.fold_in(jax.random.fold_in(rng, 6), axis_at), (blocks,), jnp.float32, smallest / len(split), high / len(split))
        gain = gain * jnp.repeat(jnp.exp(heights), dims[axis_at] // blocks).reshape((-1,) + (1,) * (len(dims) - 1 - axis_at))
    return gain


def deal_out(stream_key, own, number, rows, count, top, limit, lean):
    sequence = jax.random.permutation(stream_key, count)
    packed, usual = shares(count, rows * top, limit, lean, True), shares(count, rows * top, limit, lean, False)
    places = jnp.arange(count)

    def named(sizes, offset_by):
        used = int((sizes > 0).sum())
        fixed = max(1, used // 4)
        shifted = fixed + (places - fixed + offset_by * (used - fixed)) % max(1, count - fixed)
        return jnp.zeros((count,), jnp.int32).at[sequence[jnp.where(places < fixed, places, shifted)]].set(jnp.asarray(sizes, jnp.int32))

    sizes = jnp.where(number % 4 == 0, named(packed, number // 4), named(usual, number - number // 4 - 1))
    mixed = jax.random.permutation(jax.random.fold_in(own, 3), count)
    source_of, taker = mixed[0:count // 2 * 2:2], mixed[1:count // 2 * 2:2]
    margin = jnp.minimum(sizes[source_of] - 1, limit - sizes[taker]) // 2
    margin = jnp.where((source_of == sequence[0]) | (taker == sequence[0]) | (sizes[taker] == 0), 0, jnp.maximum(margin, 0))
    shifted = jax.random.randint(jax.random.fold_in(own, 4), (count // 2,), 0, 1 << 20) % (margin + 1)
    sizes = sizes.at[source_of].add(-shifted).at[taker].add(shifted)
    labels = jnp.searchsorted(jnp.cumsum(sizes), jnp.arange(rows * top), side="right").astype(jnp.int32)
    listing = labels.reshape(top, rows).T
    listing = listing[jax.random.permutation(jax.random.fold_in(own, 1), rows)]
    offset_by = jax.random.randint(jax.random.fold_in(own, 2), (rows, 1), 0, top)
    return jnp.take_along_axis(listing, (jnp.arange(top)[None, :] + offset_by) % top, axis=1)


def shares(amount, total, reach, lean, full):
    loads = [(1 << 20) // math.isqrt(rank ** lean) + 1 for rank in range(1, amount + 1)]
    largest = reach if full else min(reach, max(-(-total // amount), total * loads[0] // sum(loads)))
    least = 1 if total - largest >= amount - 1 else 0
    given, rest = [largest] + [least] * (amount - 1), total - largest - least * (amount - 1)
    while rest > 0:
        movable = [i for i in range(1, amount) if given[i] < largest] or [i for i in range(1, amount) if given[i] < reach]
        mass, remaining = sum([loads[i] for i in movable]), rest
        for i in movable:
            more = min(reach - given[i], max(1, remaining * loads[i] // mass), rest)
            given[i] = given[i] + more
            rest = rest - more
    return np.array(given)


def normal_values(key, extent, width, reach, shards=(), kind=jnp.bfloat16):
    loudness = levels(key, extent, shards, -0.22, 0.18) if shards else 1.0
    array = jax.random.normal(key, extent, jnp.float32) * width * loudness
    return jnp.minimum(jnp.maximum(array, -reach), reach).astype(kind)


def setup_inputs(seed: int = 0) -> dict:
    arg_keys = jax.random.split(jax.random.key(seed), 6)
    tokens = normal_values(arg_keys[0], (TOKENS, D), 1.0, 6.0, ((0, 32),))
    expert_ids_keys = jax.random.split(jax.random.fold_in(arg_keys[1], 1), TOKENS // TOK_DEV)
    expert_ids_turns = jax.random.permutation(jax.random.fold_in(arg_keys[1], 3), TOKENS // TOK_DEV)
    expert_ids = jax.vmap(lambda own, number: deal_out(jax.random.fold_in(arg_keys[1], 2), own, number, TOK_DEV, EXPERTS, TOP, CAP, 1))(expert_ids_keys, expert_ids_turns).reshape((TOKENS, TOP))
    route_probs = jnp.clip(jnp.exp(math.log(1.0) - 2.9957323 * jax.random.uniform(arg_keys[2], (TOKENS, TOP), jnp.float32) ** levels(arg_keys[2], (TOKENS, TOP), ((0, 32),), -0.2, 0.2)), 0.05, 1.0)
    w_gate_up = normal_values(arg_keys[3], (EXPERTS, D, 2 * FF), D ** -0.5, 0.125, ((0, 8), (1, 4)))
    w_down = normal_values(arg_keys[4], (EXPERTS, FF, D), FF ** -0.5, 0.21875, ((0, 8), (2, 4)))
    return {"tokens": tokens, "expert_ids": expert_ids, "route_probs": route_probs, "w_gate_up": w_gate_up, "w_down": w_down}


def reference(tokens, expert_ids, route_probs, w_gate_up, w_down):
    experts = w_gate_up.shape[0]
    device_count = tokens.shape[0] // TOK_DEV
    slots_all = device_count * CAP
    weights = route_probs / jnp.sum(route_probs, axis=1, keepdims=True)
    blocks = expert_ids.reshape(device_count, TOK_DEV * TOP).astype(jnp.int32)
    onehot = (blocks[:, :, None] == jnp.arange(experts, dtype=jnp.int32)[None, None, :]).astype(jnp.int32)
    before = jnp.cumsum(onehot, axis=1) - onehot
    slot_of = jnp.sum(before * onehot, axis=2).astype(jnp.int32)
    device_of = jnp.arange(device_count, dtype=jnp.int32)[:, None]
    position = (blocks * slots_all + device_of * CAP + slot_of).reshape(-1).astype(jnp.int32)
    token_of = (device_of * TOK_DEV + jnp.arange(TOK_DEV * TOP, dtype=jnp.int32)[None, :] // TOP).reshape(-1).astype(jnp.int32)
    row_table = jnp.zeros((experts * slots_all,), jnp.int32).at[position].set(token_of).reshape(experts, slots_all)
    row_weight = jnp.zeros((experts * slots_all,), jnp.float32).at[position].set(weights.reshape(-1).astype(jnp.float32)).reshape(experts, slots_all)

    def expert_step(running, inputs):
        rows_index, rows_scale, gate_up, down = inputs
        rows_in = tokens[rows_index]
        joined = jnp.dot(rows_in, gate_up, preferred_element_type=jnp.float32)
        hidden = (jax.nn.silu(joined[:, :FF]) * joined[:, FF:]).astype(jnp.bfloat16)
        result = jnp.dot(hidden, down, preferred_element_type=jnp.float32).astype(jnp.bfloat16)
        result = lax.optimization_barrier(result).astype(jnp.float32)
        return running.at[rows_index].add(result * rows_scale[:, None]), None

    start_sum = jnp.zeros(tokens.shape, jnp.float32)
    summed, unused = lax.scan(expert_step, start_sum, (row_table, row_weight, w_gate_up, w_down))
    return summed.astype(jnp.bfloat16)
```

```python
import functools

import jax
import jax.numpy as jnp
from jax import lax
from jax.experimental import pallas as pl
from jax.experimental.pallas import tpu as pltpu
from jax.sharding import PartitionSpec as P

MESH = pl.DeviceIdType.MESH


def xor(index, mask):
    width = 1
    while width <= mask:
        if mask & width:
            index = index + width * (1 - 2 * lax.rem(index // width, 2))
        width *= 2
    return index


def span(masks):
    out = [0]
    for m in masks:
        out = out + [m ^ s for s in out]
    return out


class Gather:
    def __init__(self, orders, me, target, own, slot, send_sem, recv_sem):
        self.orders, self.me, self.target = orders, me, target
        self.own, self.slot = own, slot
        self.send_sem, self.recv_sem = send_sem, recv_sem
        self.started = []

    def stages(self):
        return len(self.orders[0])

    def send(self, stage):
        for half, order in enumerate(self.orders):
            g = order[stage]
            for s in span(order[:stage]):
                block = xor(self.me, s)
                dst = self.slot(block, half)
                copy = pltpu.make_async_remote_copy(
                    src_ref=self.own(half) if s == 0 else dst,
                    dst_ref=dst,
                    send_sem=self.send_sem.at[half, g ^ s],
                    recv_sem=self.recv_sem.at[half, g ^ s],
                    device_id=self.target(xor(self.me, g)),
                    device_id_type=MESH,
                )
                copy.start()
                self.started.append(copy)

    def wait(self, stage):
        for half, order in enumerate(self.orders):
            g = order[stage]
            for s in span(order[:stage]):
                ref = self.slot(xor(self.me, g ^ s), half)
                pltpu.make_async_remote_copy(
                    src_ref=ref,
                    dst_ref=ref,
                    send_sem=self.send_sem.at[half, g ^ s],
                    recv_sem=self.recv_sem.at[half, g ^ s],
                    device_id=self.target(xor(self.me, g)),
                    device_id_type=MESH,
                ).wait_recv()

    def drain(self):
        for copy in self.started:
            copy.wait_send()


def powers(count):
    out, width = [], 1
    while width < count:
        out.append(width)
        width *= 2
    return out


def kernel(
    dps, owners,
    tok_in, share_in, gu_in, dn_in, got,
    tok, share, gu, dn, hid, sib,
    tok_s, tok_r, share_s, share_r, gu_s, gu_r, dn_s, dn_r, sib_s, sib_r, out_s, out_r, loc,
):
    dp, ex = lax.axis_index("dp"), lax.axis_index("expert")
    chips = owners // 2
    chip, core = ex // 2, lax.rem(ex, 2)
    local = gu_in.shape[0]
    depth = gu_in.shape[1]
    cols = dn_in.shape[2]
    rows, width = tok_in.shape
    ff = dn_in.shape[1]

    dp_masks = powers(dps)
    chip_masks = [2 * (2 * w - 1) for w in powers(chips)]

    barrier = pltpu.get_barrier_semaphore()
    peers = [(xor(dp, m), ex) for m in dp_masks] + [(dp, xor(ex, r)) for r in range(1, owners)]
    for peer in peers:
        pl.semaphore_signal(barrier, inc=1, device_id=peer, device_id_type=MESH)
    pl.semaphore_wait(barrier, len(peers))

    def on_expert(index):
        return (dp, index)

    def on_dp(index):
        return (index, ex)

    half_rows, half_depth, half_ff = rows // 2, depth // 2, ff // 2
    tokens = Gather(
        [chip_masks + [1], chip_masks[::-1] + [1]], ex, on_expert,
        lambda h: tok_in.at[pl.ds(h * half_rows, half_rows)],
        lambda b, h: tok.at[b // 2, lax.rem(b, 2), pl.ds(h * half_rows, half_rows)],
        tok_s, tok_r,
    )
    ups = [
        Gather(
            [dp_masks, dp_masks[::-1]], dp, on_dp,
            lambda h, e=e: gu_in.at[e, pl.ds(h * half_depth, half_depth)],
            lambda b, h, e=e: gu.at[e, pl.ds(pl.multiple_of(b * depth + h * half_depth, half_depth), half_depth)],
            gu_s.at[e], gu_r.at[e],
        )
        for e in range(local)
    ]
    down = Gather(
        [dp_masks, dp_masks[::-1]], dp, on_dp,
        lambda h: dn_in.at[:, pl.ds(h * half_ff, half_ff)],
        lambda b, h: dn.at[b, :, pl.ds(h * half_ff, half_ff)],
        dn_s, dn_r,
    )

    tokens.send(0)
    for e in range(local):
        ups[e].send(0)
    shares = []
    for r in range(1, owners):
        copy = pltpu.make_async_remote_copy(
            src_ref=share_in.at[xor(ex, r)], dst_ref=share.at[ex],
            send_sem=share_s.at[r], recv_sem=share_r.at[r],
            device_id=(dp, xor(ex, r)), device_id_type=MESH,
        )
        copy.start()
        shares.append(copy)
    locals_ = [
        pltpu.make_async_copy(tok_in, tok.at[chip, core], loc.at[0]),
        pltpu.make_async_copy(share_in.at[ex], share.at[ex], loc.at[1]),
        pltpu.make_async_copy(
            gu_in, gu.at[:, pl.ds(pl.multiple_of(dp * depth, depth), depth)], loc.at[2]
        ),
        pltpu.make_async_copy(dn_in, dn.at[dp], loc.at[3]),
    ]
    for copy in locals_:
        copy.start()

    last = len(dp_masks) - 1
    queue = [(g, stage) for g in ups for stage in range(1, last + 1)]
    tok_stage, tok_last = 0, tokens.stages() - 1

    def step_tokens():
        nonlocal tok_stage
        if tok_stage < tok_last:
            tokens.wait(tok_stage)
            tok_stage += 1
            tokens.send(tok_stage)

    for at, (g, stage) in enumerate(queue):
        step_tokens()
        g.wait(stage - 1)
        g.send(stage)
        if at == 0:
            down.send(0)
    while tok_stage < tok_last:
        step_tokens()
    tokens.wait(tok_last)
    for copy in locals_:
        copy.wait()

    tile = 256 if ff % 256 == 0 else ff

    def hidden(e):
        def body(c, carry):
            x = tok[c].reshape(2 * rows, width)
            for f in range(ff // tile):
                a = jnp.dot(x, gu[e, :, f * tile:(f + 1) * tile], preferred_element_type=jnp.float32)
                b = jnp.dot(
                    x, gu[e, :, ff + f * tile:ff + (f + 1) * tile], preferred_element_type=jnp.float32
                )
                hid[e, c, :, f * tile:(f + 1) * tile] = (a / (1.0 + jnp.exp(-a)) * b).astype(hid.dtype)
            return carry

        lax.fori_loop(0, chips, body, 0)

    for e in range(local):
        ups[e].wait(last)
        hidden(e)
        if e == 0:
            for stage in range(1, last + 1):
                down.wait(stage - 1)
                down.send(stage)

    tokens.drain()
    for r, copy in enumerate(shares):
        pltpu.make_async_remote_copy(
            src_ref=share_in.at[0], dst_ref=share.at[xor(ex, r + 1)],
            send_sem=share_s.at[r + 1], recv_sem=share_r.at[r + 1],
            device_id=(dp, xor(ex, r + 1)), device_id_type=MESH,
        ).wait_recv()

    def partial(b):
        at = pl.ds(pl.multiple_of(b * cols, cols), cols)

        def body(c, carry):
            parts = [
                jnp.dot(hid[e, c], dn[b, e], preferred_element_type=jnp.float32) for e in range(local)
            ]
            for k in range(2):
                scale = jnp.transpose(share[2 * c + k])
                total = parts[0][k * rows:(k + 1) * rows] * scale[:, 0:1]
                for e in range(1, local):
                    total = total + parts[e][k * rows:(k + 1) * rows] * scale[:, e:e + 1]
                tok[c, k, :, at] = total.astype(tok.dtype)
            return carry

        lax.fori_loop(0, chips, body, 0)

    def to_sibling(s, b):
        at = pl.ds(pl.multiple_of(b * cols, cols), cols)
        copy = pltpu.make_async_remote_copy(
            src_ref=tok.at[:, 1 - core, :, at], dst_ref=sib.at[:, :, at],
            send_sem=sib_s.at[s], recv_sem=sib_r.at[s],
            device_id=(dp, xor(ex, 1)), device_id_type=MESH,
        )
        return copy

    sent = []

    def combine(s, b):
        at = pl.ds(pl.multiple_of(b * cols, cols), cols)

        def body(c, carry):
            tok[c, core, :, at] = (
                tok[c, core, :, at].astype(jnp.float32) + sib[c, :, at].astype(jnp.float32)
            ).astype(tok.dtype)
            return carry

        lax.fori_loop(0, chips, body, 0)
        for r in range(1, chips):
            other = xor(chip, r)
            copy = pltpu.make_async_remote_copy(
                src_ref=tok.at[other, core, :, at], dst_ref=got.at[chip, :, at],
                send_sem=out_s.at[s, r], recv_sem=out_r.at[s, r],
                device_id=(dp, xor(ex, 2 * r)), device_id_type=MESH,
            )
            copy.start()
            sent.append(copy)
        own = pltpu.make_async_copy(tok.at[chip, core, :, at], got.at[chip, :, at], out_r.at[s, 0])
        own.start()
        sent.append(own)

    pending = None
    for s in range(dps):
        b = xor(dp, s)
        if s == 1:
            down.wait(last)
        partial(b)
        copy = to_sibling(s, b)
        copy.start()
        if pending is not None:
            pending[2].wait()
            combine(pending[0], pending[1])
        pending = (s, b, copy)
    pending[2].wait()
    combine(pending[0], pending[1])

    for s in range(dps):
        b = xor(dp, s)
        at = pl.ds(pl.multiple_of(b * cols, cols), cols)
        for r in range(1, chips):
            pltpu.make_async_remote_copy(
                src_ref=tok.at[chip, core, :, at], dst_ref=got.at[xor(chip, r), :, at],
                send_sem=out_s.at[s, r], recv_sem=out_r.at[s, r],
                device_id=(dp, xor(ex, 2 * r)), device_id_type=MESH,
            ).wait_recv()
    for at, copy in enumerate(sent):
        if at % chips == chips - 1:
            copy.wait()
        else:
            copy.wait_send()
    for copy in shares:
        copy.wait_send()
    for g in ups + [down]:
        g.drain()


def shards(tokens, expert_ids, route_probs, w_gate_up, w_down):
    dps, owners = lax.axis_size("dp"), lax.axis_size("expert")
    chips = owners // 2
    local, depth, both = w_gate_up.shape
    experts = owners * local
    rows, width = tokens.shape
    ff, cols = w_down.shape[1:]
    weights = route_probs / jnp.sum(route_probs, axis=1, keepdims=True)
    share = jnp.sum(
        jnp.where(
            expert_ids.T[None] == jnp.arange(experts, dtype=jnp.int32)[:, None, None],
            weights.T[None], 0.0,
        ),
        axis=1,
    ).reshape(owners, local, rows)
    pad = -local % 8
    share = jnp.pad(share, ((0, 0), (0, pad), (0, 0)))
    any_ = pl.BlockSpec(memory_space=pl.ANY)
    dma = pltpu.SemaphoreType.DMA
    bf16 = jnp.bfloat16
    got = pl.pallas_call(
        functools.partial(kernel, dps, owners),
        out_shape=jax.ShapeDtypeStruct((chips, rows, width), bf16),
        in_specs=[any_] * 4,
        out_specs=any_,
        scratch_shapes=[
            pltpu.VMEM((chips, 2, rows, width), bf16),
            pltpu.VMEM((owners, local + pad, rows), jnp.float32),
            pltpu.VMEM((local, dps * depth, both), bf16),
            pltpu.VMEM((dps, local, ff, cols), bf16),
            pltpu.VMEM((local, chips, 2 * rows, ff), bf16),
            pltpu.VMEM((chips, rows, width), bf16),
            dma((2, owners)), dma((2, owners)),
            dma((owners,)), dma((owners,)),
            dma((local, 2, dps)), dma((local, 2, dps)),
            dma((2, dps)), dma((2, dps)),
            dma((dps,)), dma((dps,)),
            dma((dps, chips)), dma((dps, chips)),
            dma((4,)),
        ],
        compiler_params=pltpu.CompilerParams(
            collective_id=0, has_side_effects=True, vmem_limit_bytes=67043328
        ),
    )(tokens, share, w_gate_up, w_down)
    return jnp.sum(got.astype(jnp.float32), axis=0).astype(bf16)


def solution(mesh):
    return jax.shard_map(
        shards,
        mesh=mesh,
        in_specs=(
            P(("dp", "expert"), None),
            P(("dp", "expert"), None),
            P(("dp", "expert"), None),
            P("expert", "dp", None),
            P("expert", None, "dp"),
        ),
        out_specs=P(("dp", "expert"), None),
        check_vma=False,
    )
```

```python
import functools

import jax
import jax.numpy as jnp
from jax import lax
from jax.experimental import pallas as pl
from jax.experimental.pallas import tpu as pltpu
from jax.sharding import PartitionSpec as P

MESH = pl.DeviceIdType.MESH


def xor(index, mask):
    width = 1
    while width <= mask:
        if mask & width:
            index = index + width * (1 - 2 * lax.rem(index // width, 2))
        width *= 2
    return index


def span(masks):
    out = [0]
    for m in masks:
        out = out + [m ^ s for s in out]
    return out


class Gather:
    def __init__(self, orders, me, target, own, slot, send_sem, recv_sem):
        self.orders, self.me, self.target = orders, me, target
        self.own, self.slot = own, slot
        self.send_sem, self.recv_sem = send_sem, recv_sem
        self.started = []

    def stages(self):
        return len(self.orders[0])

    def send(self, stage):
        for half, order in enumerate(self.orders):
            g = order[stage]
            for s in span(order[:stage]):
                block = xor(self.me, s)
                dst = self.slot(block, half)
                copy = pltpu.make_async_remote_copy(
                    src_ref=self.own(half) if s == 0 else dst,
                    dst_ref=dst,
                    send_sem=self.send_sem.at[half, g ^ s],
                    recv_sem=self.recv_sem.at[half, g ^ s],
                    device_id=self.target(xor(self.me, g)),
                    device_id_type=MESH,
                )
                copy.start()
                self.started.append(copy)

    def wait(self, stage):
        for half, order in enumerate(self.orders):
            g = order[stage]
            for s in span(order[:stage]):
                ref = self.slot(xor(self.me, g ^ s), half)
                pltpu.make_async_remote_copy(
                    src_ref=ref,
                    dst_ref=ref,
                    send_sem=self.send_sem.at[half, g ^ s],
                    recv_sem=self.recv_sem.at[half, g ^ s],
                    device_id=self.target(xor(self.me, g)),
                    device_id_type=MESH,
                ).wait_recv()

    def drain(self):
        for copy in self.started:
            copy.wait_send()


def powers(count):
    out, width = [], 1
    while width < count:
        out.append(width)
        width *= 2
    return out


def kernel(
    dps, owners,
    tok_in, share_in, gu_in, dn_in, got,
    tok, share, gu, dn, hid, sib, near,
    tok_s, tok_r, share_s, share_r, gu_s, gu_r, dn_s, dn_r, sib_s, sib_r, near_s, near_r, out_s, out_r, loc,
):
    dp, ex = lax.axis_index("dp"), lax.axis_index("expert")
    chips, pairs = owners // 2, owners // 4
    chip, core = ex // 2, lax.rem(ex, 2)
    pair, side = chip // 2, lax.rem(chip, 2)
    local = gu_in.shape[0]
    depth = gu_in.shape[1]
    cols = dn_in.shape[2]
    rows, width = tok_in.shape
    ff = dn_in.shape[1]

    dp_masks = powers(dps)
    chip_masks = [2 * (2 * w - 1) for w in powers(chips)]

    barrier = pltpu.get_barrier_semaphore()
    peers = [(xor(dp, m), ex) for m in dp_masks] + [(dp, xor(ex, r)) for r in range(1, owners)]
    for peer in peers:
        pl.semaphore_signal(barrier, inc=1, device_id=peer, device_id_type=MESH)
    pl.semaphore_wait(barrier, len(peers))

    def on_expert(index):
        return (dp, index)

    def on_dp(index):
        return (index, ex)

    half_rows, half_depth, half_ff = rows // 2, depth // 2, ff // 2
    tokens = Gather(
        [chip_masks + [1], chip_masks[::-1] + [1]], ex, on_expert,
        lambda h: tok_in.at[pl.ds(h * half_rows, half_rows)],
        lambda b, h: tok.at[b // 4, lax.rem(b // 2, 2), lax.rem(b, 2), pl.ds(h * half_rows, half_rows)],
        tok_s, tok_r,
    )
    ups = [
        Gather(
            [dp_masks, dp_masks[::-1]], dp, on_dp,
            lambda h, e=e: gu_in.at[e, pl.ds(h * half_depth, half_depth)],
            lambda b, h, e=e: gu.at[e, pl.ds(pl.multiple_of(b * depth + h * half_depth, half_depth), half_depth)],
            gu_s.at[e], gu_r.at[e],
        )
        for e in range(local)
    ]
    down = Gather(
        [dp_masks, dp_masks[::-1]], dp, on_dp,
        lambda h: dn_in.at[:, pl.ds(h * half_ff, half_ff)],
        lambda b, h: dn.at[b, :, pl.ds(h * half_ff, half_ff)],
        dn_s, dn_r,
    )

    tokens.send(0)
    for e in range(local):
        ups[e].send(0)
    shares = []
    for r in range(1, owners):
        copy = pltpu.make_async_remote_copy(
            src_ref=share_in.at[xor(ex, r)], dst_ref=share.at[ex],
            send_sem=share_s.at[r], recv_sem=share_r.at[r],
            device_id=(dp, xor(ex, r)), device_id_type=MESH,
        )
        copy.start()
        shares.append(copy)
    locals_ = [
        pltpu.make_async_copy(tok_in, tok.at[pair, side, core], loc.at[0]),
        pltpu.make_async_copy(share_in.at[ex], share.at[ex], loc.at[1]),
        pltpu.make_async_copy(
            gu_in, gu.at[:, pl.ds(pl.multiple_of(dp * depth, depth), depth)], loc.at[2]
        ),
        pltpu.make_async_copy(dn_in, dn.at[dp], loc.at[3]),
    ]
    for copy in locals_:
        copy.start()

    last = len(dp_masks) - 1
    queue = [(g, stage) for g in ups for stage in range(1, last + 1)]
    tok_stage, tok_last = 0, tokens.stages() - 1

    def step_tokens():
        nonlocal tok_stage
        if tok_stage < tok_last:
            tokens.wait(tok_stage)
            tok_stage += 1
            tokens.send(tok_stage)

    for at, (g, stage) in enumerate(queue):
        step_tokens()
        g.wait(stage - 1)
        g.send(stage)
    down.send(0)
    while tok_stage < tok_last:
        step_tokens()
    tokens.wait(tok_last)
    for copy in locals_:
        copy.wait()

    tile = 256 if ff % 256 == 0 else ff

    def hidden(e):
        def body(c, carry):
            x = tok[c // 2, lax.rem(c, 2)].reshape(2 * rows, width)
            for f in range(ff // tile):
                a = jnp.dot(x, gu[e, :, f * tile:(f + 1) * tile], preferred_element_type=jnp.float32)
                b = jnp.dot(
                    x, gu[e, :, ff + f * tile:ff + (f + 1) * tile], preferred_element_type=jnp.float32
                )
                hid[e, c, :, f * tile:(f + 1) * tile] = (a / (1.0 + jnp.exp(-a)) * b).astype(hid.dtype)
            return carry

        lax.fori_loop(0, chips, body, 0)

    for e in range(local):
        ups[e].wait(last)
        hidden(e)
        if e == 0:
            for stage in range(1, last + 1):
                down.wait(stage - 1)
                down.send(stage)

    tokens.drain()
    for r, copy in enumerate(shares):
        pltpu.make_async_remote_copy(
            src_ref=share_in.at[0], dst_ref=share.at[xor(ex, r + 1)],
            send_sem=share_s.at[r + 1], recv_sem=share_r.at[r + 1],
            device_id=(dp, xor(ex, r + 1)), device_id_type=MESH,
        ).wait_recv()

    def partial(b):
        at = pl.ds(pl.multiple_of(b * cols, cols), cols)

        def body(c, carry):
            parts = [
                jnp.dot(hid[e, c], dn[b, e], preferred_element_type=jnp.float32) for e in range(local)
            ]
            for k in range(2):
                scale = jnp.transpose(share[2 * c + k])
                total = parts[0][k * rows:(k + 1) * rows] * scale[:, 0:1]
                for e in range(1, local):
                    total = total + parts[e][k * rows:(k + 1) * rows] * scale[:, e:e + 1]
                tok[c // 2, lax.rem(c, 2), k, :, at] = total.astype(tok.dtype)
            return carry

        lax.fori_loop(0, chips, body, 0)

    def to_sibling(s, b):
        at = pl.ds(pl.multiple_of(b * cols, cols), cols)
        copy = pltpu.make_async_remote_copy(
            src_ref=tok.at[:, :, 1 - core, :, at], dst_ref=sib.at[:, :, :, at],
            send_sem=sib_s.at[s], recv_sem=sib_r.at[s],
            device_id=(dp, xor(ex, 1)), device_id_type=MESH,
        )
        return copy

    def add(c, side_, ref, at):
        tok[c, side_, core, :, at] = (
            tok[c, side_, core, :, at].astype(jnp.float32) + ref[...].astype(jnp.float32)
        ).astype(tok.dtype)

    def to_near(s, b):
        at = pl.ds(pl.multiple_of(b * cols, cols), cols)

        def body(c, carry):
            add(c, 1 - side, sib.at[c, 1 - side, :, at], at)
            return carry

        lax.fori_loop(0, pairs, body, 0)

        def body_own(c, carry):
            add(c, side, sib.at[c, side, :, at], at)
            return carry

        lax.fori_loop(0, pairs, body_own, 0)
        return pltpu.make_async_remote_copy(
            src_ref=tok.at[:, 1 - side, core, :, at], dst_ref=near.at[:, :, at],
            send_sem=near_s.at[s], recv_sem=near_r.at[s],
            device_id=(dp, xor(ex, 2)), device_id_type=MESH,
        )

    sent = []

    def home(s, b):
        at = pl.ds(pl.multiple_of(b * cols, cols), cols)

        def body(c, carry):
            add(c, side, near.at[c, :, at], at)
            return carry

        lax.fori_loop(0, pairs, body, 0)
        for r in range(1, pairs):
            copy = pltpu.make_async_remote_copy(
                src_ref=tok.at[xor(pair, r), side, core, :, at], dst_ref=got.at[pair, :, at],
                send_sem=out_s.at[s, r], recv_sem=out_r.at[s, r],
                device_id=(dp, xor(ex, 4 * r)), device_id_type=MESH,
            )
            copy.start()
            sent.append(copy)
        own = pltpu.make_async_copy(tok.at[pair, side, core, :, at], got.at[pair, :, at], out_r.at[s, 0])
        own.start()
        sent.append(own)

    first, second = {}, {}
    for s in range(dps + 2):
        if s < dps:
            if s == 1:
                down.wait(last)
            partial(xor(dp, s))
            first[s] = to_sibling(s, xor(dp, s))
            first[s].start()
        if 1 <= s < dps + 1:
            first[s - 1].wait()
            second[s - 1] = to_near(s - 1, xor(dp, s - 1))
            second[s - 1].start()
        if s >= 2:
            second[s - 2].wait()
            home(s - 2, xor(dp, s - 2))

    for s in range(dps):
        b = xor(dp, s)
        at = pl.ds(pl.multiple_of(b * cols, cols), cols)
        for r in range(1, pairs):
            pltpu.make_async_remote_copy(
                src_ref=tok.at[pair, side, core, :, at], dst_ref=got.at[xor(pair, r), :, at],
                send_sem=out_s.at[s, r], recv_sem=out_r.at[s, r],
                device_id=(dp, xor(ex, 4 * r)), device_id_type=MESH,
            ).wait_recv()
    for at, copy in enumerate(sent):
        if at % pairs == pairs - 1:
            copy.wait()
        else:
            copy.wait_send()
    for copy in shares:
        copy.wait_send()
    for g in ups + [down]:
        g.drain()


def shards(tokens, expert_ids, route_probs, w_gate_up, w_down):
    dps, owners = lax.axis_size("dp"), lax.axis_size("expert")
    chips, pairs = owners // 2, owners // 4
    local, depth, both = w_gate_up.shape
    experts = owners * local
    rows, width = tokens.shape
    ff, cols = w_down.shape[1:]
    weights = route_probs / jnp.sum(route_probs, axis=1, keepdims=True)
    share = jnp.sum(
        jnp.where(
            expert_ids.T[None] == jnp.arange(experts, dtype=jnp.int32)[:, None, None],
            weights.T[None], 0.0,
        ),
        axis=1,
    ).reshape(owners, local, rows)
    pad = -local % 8
    share = jnp.pad(share, ((0, 0), (0, pad), (0, 0)))
    any_ = pl.BlockSpec(memory_space=pl.ANY)
    dma = pltpu.SemaphoreType.DMA
    bf16 = jnp.bfloat16
    got = pl.pallas_call(
        functools.partial(kernel, dps, owners),
        out_shape=jax.ShapeDtypeStruct((pairs, rows, width), bf16),
        in_specs=[any_] * 4,
        out_specs=any_,
        scratch_shapes=[
            pltpu.VMEM((pairs, 2, 2, rows, width), bf16),
            pltpu.VMEM((owners, local + pad, rows), jnp.float32),
            pltpu.VMEM((local, dps * depth, both), bf16),
            pltpu.VMEM((dps, local, ff, cols), bf16),
            pltpu.VMEM((local, chips, 2 * rows, ff), bf16),
            pltpu.VMEM((pairs, 2, rows, width), bf16),
            pltpu.VMEM((pairs, rows, width), bf16),
            dma((2, owners)), dma((2, owners)),
            dma((owners,)), dma((owners,)),
            dma((local, 2, dps)), dma((local, 2, dps)),
            dma((2, dps)), dma((2, dps)),
            dma((dps,)), dma((dps,)),
            dma((dps,)), dma((dps,)),
            dma((dps, pairs)), dma((dps, pairs)),
            dma((4,)),
        ],
        compiler_params=pltpu.CompilerParams(
            collective_id=0, has_side_effects=True, vmem_limit_bytes=67043328
        ),
    )(tokens, share, w_gate_up, w_down)
    return jnp.sum(got.astype(jnp.float32), axis=0).astype(bf16)


def solution(mesh):
    return jax.shard_map(
        shards,
        mesh=mesh,
        in_specs=(
            P(("dp", "expert"), None),
            P(("dp", "expert"), None),
            P(("dp", "expert"), None),
            P("expert", "dp", None),
            P("expert", None, "dp"),
        ),
        out_specs=P(("dp", "expert"), None),
        check_vma=False,
    )
```
